16 devices in a mesh: rep: 1, r: 4 (over y, z), s: 4 (over x, core).
Axes of the slice: x: 2, y: 2, z: 2, core: 2. Of those that a mesh axis runs over, the one named last changes fastest.
Arguments:
- x: bfloat16 [16, 4096, 896], P(('rep', 'r', 's'))
- dy: bfloat16 [16, 4096, 896], P(('rep', 'r', 's'))
- w_gate: bfloat16 [2, 896, 2560], P(None, 's')
- w_up: bfloat16 [2, 896, 2560], P(None, 's')
- w_down: bfloat16 [2, 2560, 896], P(None, 's')
- m_w_gate: float32 [2, 896, 2560], P(None, 's')
- m_w_up: float32 [2, 896, 2560], P(None, 's')
- m_w_down: float32 [2, 2560, 896], P(None, 's')
- v_w_gate: float32 [2, 896, 2560], P(None, 's')
- v_w_up: float32 [2, 896, 2560], P(None, 's')
- v_w_down: float32 [2, 2560, 896], P(None, 's')
Outputs:
- output 1: bfloat16 [2, 896, 2560], P('rep', 's')
- output 2: bfloat16 [2, 896, 2560], P('rep', 's')
- output 3: bfloat16 [2, 2560, 896], P('rep', 's')
- output 4: float32 [2, 896, 2560], P('rep', 's')
- output 5: float32 [2, 896, 2560], P('rep', 's')
- output 6: float32 [2, 2560, 896], P('rep', 's')
- output 7: float32 [2, 896, 2560], P('rep', 's')
- output 8: float32 [2, 896, 2560], P('rep', 's')
- output 9: float32 [2, 2560, 896], P('rep', 's')
All inputs are finite; a program needn't handle non-finite values.
Results may differ from the reference program's by a relative error of at most 0.02.
Values are sent between devices in bfloat16 or wider.
A program may use at most 2 GiB of HBM per device.

```python
import jax
import jax.numpy as jnp
from jax import lax

SEQUENCES = 16
TOKENS = 4096
D = 896
FF = 2560
LAYERS = 2
NAMES = ("w_gate", "w_up", "w_down")
SHAPES = {"w_gate": (LAYERS, D, FF), "w_up": (LAYERS, D, FF), "w_down": (LAYERS, FF, D)}


def bump(key, n, height):
    away = (jnp.arange(n, dtype=jnp.int32) - jax.random.randint(key, (), 0, n, jnp.int32)) % n
    return jnp.where(away < n // 8, height, 1.0)


def together(key, own, strength):
    shared = jax.random.normal(key, own.shape[1:], jnp.float32)
    return (own + strength * shared) * lax.rsqrt(1 + strength * strength)


def setup_inputs(seed: int = 0, part: int = 0) -> dict:
    kx, kdy, ka, kb, kz, kf, kh, kl, *keys = jax.random.split(jax.random.key(seed), 8 + 3 * len(NAMES))
    kx, kdy, ka, kb = (jax.random.fold_in(k, part) for k in (kx, kdy, ka, kb))
    kw, km, kv = (keys[i::3] for i in range(3))
    shape = (SEQUENCES, TOKENS, D)
    much_x, much_dy = jax.random.uniform(kz, (2,), jnp.float32, 0.0, 1.0)
    loud = 2.0 ** jax.random.uniform(jax.random.fold_in(kz, 1), (), jnp.float32, -1.0, 2.0)
    layers = 2.0 ** jax.random.uniform(kl, (LAYERS, 1, 1), jnp.float32, -1.0, 1.0)
    x = together(ka, jax.random.normal(kx, shape, jnp.float32), much_x) * bump(kf, D, 4.0)
    dy = together(kb, jax.random.normal(kdy, shape, jnp.float32), much_dy)
    drawn = {"x": x.astype(jnp.bfloat16), "dy": (loud * dy * (SEQUENCES * TOKENS) ** -0.5).astype(jnp.bfloat16)}
    for key, name in zip(kw, NAMES, strict=True):
        w = jax.random.normal(key, SHAPES[name], jnp.float32) * SHAPES[name][1] ** -0.5
        drawn[name] = (w * {"w_gate": 1.0, "w_up": bump(kh, FF, 4.0), "w_down": layers}[name]).astype(jnp.bfloat16)
    for key, name in zip(km, NAMES, strict=True):
        drawn[f"m_{name}"] = 0.1 * jax.random.normal(key, SHAPES[name], jnp.float32)
    for key, name in zip(kv, NAMES, strict=True):
        drawn[f"v_{name}"] = jax.random.uniform(key, SHAPES[name], jnp.float32, 0.005, 0.015)
    return drawn


def matmul(a, w):
    return jnp.dot(a, w, preferred_element_type=jnp.float32).astype(jnp.bfloat16)


def normed(h):
    wide = h.astype(jnp.float32)
    scale = lax.rsqrt(jnp.mean(wide**2, -1, keepdims=True) + 1e-6)
    return (wide * scale).astype(jnp.bfloat16)


def layer(h, w):
    a = normed(h)
    gate = jnp.dot(a, w["w_gate"], preferred_element_type=jnp.float32)
    up = jnp.dot(a, w["w_up"], preferred_element_type=jnp.float32)
    return h + matmul((jax.nn.silu(gate) * up).astype(jnp.bfloat16), w["w_down"])


def adamw(w, m, v, g):
    m = 0.9 * m + 0.1 * g
    v = 0.95 * v + 0.05 * g * g
    step = m * lax.rsqrt(v + 1e-8) + 0.1 * w
    return (w - 0.02 * step).astype(jnp.bfloat16), m, v


def stack(weights, h):
    return lax.scan(lambda h, w: (layer(h, w), None), h, weights)[0]


def reference(x, dy, w_gate, w_up, w_down, m_w_gate, m_w_up, m_w_down, v_w_gate, v_w_up, v_w_down):
    weights = dict(zip(NAMES, (w_gate, w_up, w_down), strict=True))

    def take(so_far, sequence):
        h, by_y = sequence
        _, back = jax.vjp(lambda w: stack(w, h), weights)
        return jax.tree.map(lambda total, term: total + term.astype(jnp.float32), so_far, back(by_y)[0]), None

    none_yet = {name: jnp.zeros(w.shape, jnp.float32) for name, w in weights.items()}
    by_weights, _ = lax.scan(take, none_yet, (x, dy))
    gradients = [by_weights[name].astype(jnp.bfloat16).astype(jnp.float32) for name in NAMES]
    new = [
        adamw(w.astype(jnp.float32), m, v, g)
        for w, m, v, g in zip((w_gate, w_up, w_down), (m_w_gate, m_w_up, m_w_down), (v_w_gate, v_w_up, v_w_down), gradients, strict=True)
    ]
    return tuple(one[which] for which in range(3) for one in new)
```

```python
import functools

import jax
import jax.numpy as jnp
from jax import lax
from jax.experimental import pallas as pl
from jax.experimental.pallas import tpu as pltpu
from jax.sharding import PartitionSpec as P

F32, BF16 = jnp.float32, jnp.bfloat16
TOKENS, D, FF = 4096, 896, 2560
RD, RF = D // 4, FF // 4
VMEM = 66_000_000
ANY = pl.BlockSpec(memory_space=pl.ANY)


def dot(a, b):
    return jnp.dot(a, b, preferred_element_type=F32)


def dot_t(a, b):
    return lax.dot_general(a, b, (((1,), (1,)), ((), ())), preferred_element_type=F32)


def scale_of(wide):
    return lax.rsqrt(jnp.mean(wide * wide, -1, keepdims=True) + 1e-6)


def call(kernel, name, grid, in_specs, out_specs, out_shape, scratch=(), flops=0, nbytes=0, trans=0):
    return pl.pallas_call(
        kernel,
        grid=(grid,),
        in_specs=in_specs,
        out_specs=out_specs,
        out_shape=out_shape,
        scratch_shapes=list(scratch),
        name=name,
        compiler_params=pltpu.CompilerParams(vmem_limit_bytes=VMEM, dimension_semantics=("arbitrary",)),
        cost_estimate=pl.CostEstimate(flops=flops, bytes_accessed=nbytes, transcendentals=trans),
    )


MM = 2 * TOKENS * D * FF


def shape(*dims, dtype=BF16):
    return jax.ShapeDtypeStruct(dims, dtype)


def rows(t, width):
    return pl.BlockSpec((t, width), lambda i: (i, 0))


def columns(height, t):
    return pl.BlockSpec((height, t), lambda i: (0, i))


def picked(layer, *dims):
    return pl.BlockSpec((None,) + dims, lambda i: (layer, 0, 0), pipeline_mode=pl.Buffered(1))


def whole(*dims):
    return pl.BlockSpec(dims, lambda i: (0,) * len(dims), pipeline_mode=pl.Buffered(1))


T1 = 512
SUB1 = 256


def flip1(i):
    return i + 1 - 2 * (i % 2)


def others(i):
    return i, flip1(i), (i + 2) % 4, 3 - i


def remote(src, dst, send, recv, to):
    return pltpu.make_async_remote_copy(
        src_ref=src, dst_ref=dst, send_sem=send, recv_sem=recv, device_id=to, device_id_type=pl.DeviceIdType.MESH
    )


CUT = 256


def forward_in(x, w_gate, w_up):
    cuts = FF // CUT

    def kernel(x_ref, wg_ref, wu_ref, gate_ref, up_ref, act_ref, at_ref, a_s, w_s, x_sem, own_sem, as_sem, ar_sem, bs_sem, br_sem, fs_sem, fr_sem):
        t = pl.program_id(0)
        rep, r, s = lax.axis_index("rep"), lax.axis_index("r"), lax.axis_index("s")
        near, far = (rep, r, flip1(s)), (rep, r, (s + 2) % 4)
        w_refs = (wg_ref, wu_ref)
        held = lambda i: pl.ds(pl.multiple_of(i * RD, RD), RD)
        cols = lambda c: pl.ds(pl.multiple_of(c * CUT, CUT), CUT)

        def near_copy(i):
            return remote(w_refs[i].at[0], w_s.at[i, held(s)], as_sem.at[i], ar_sem.at[i], near)

        def far_copy(i, c):
            return remote(w_refs[i].at[0, :, cols(c)], w_s.at[i, held(s), cols(c)], bs_sem.at[i, c], br_sem.at[i, c], far)

        def on_copy(i, c):
            there = w_s.at[i, held((s + 2) % 4), cols(c)]
            return remote(there, there, fs_sem.at[i, c], fr_sem.at[i, c], near)

        @pl.when(t == 0)
        def _():
            states = pltpu.make_async_copy(x_ref, a_s, x_sem)
            states.start()
            own = [pltpu.make_async_copy(w_refs[i].at[0], w_s.at[i, held(s)], own_sem.at[i]) for i in range(2)]
            for c in own:
                c.start()
            barrier = pltpu.get_barrier_semaphore()
            for to in (near, far):
                pl.semaphore_signal(barrier, inc=1, device_id=to, device_id_type=pl.DeviceIdType.MESH)
            pl.semaphore_wait(barrier, 2)

            @pl.loop(0, cuts)
            def _(c):
                for i in range(2):
                    far_copy(i, c).start()

            for i in range(2):
                near_copy(i).start()
            states.wait()
            for j in range(0, TOKENS, 512):
                wide = a_s[j : j + 512, :].astype(F32)
                a = (wide * scale_of(wide)).astype(BF16)
                a_s[j : j + 512, :] = a
                at_ref[:, j : j + 512] = a.T
            for c in own:
                c.wait()
            for i in range(2):
                near_copy(i).wait()

        @pl.when(t < cuts)
        def _():
            for i in range(2):
                far_copy(i, t).wait()
            for i in range(2):
                on_copy(i, t).start()

        @pl.when(t > 0)
        def _():
            for i in range(2):
                on_copy(i, t - 1).wait()
            wg, wu = w_s[0, :, cols(t - 1)], w_s[1, :, cols(t - 1)]
            for j in range(0, TOKENS, 512):
                a = a_s[j : j + 512, :]
                g, u = dot(a, wg), dot(a, wu)
                gate_ref[j : j + 512, :] = g
                up_ref[j : j + 512, :] = u
                act_ref[j : j + 512, :] = (g * jax.nn.sigmoid(g) * u).astype(BF16)

    dma = pltpu.SemaphoreType.DMA
    block = pl.BlockSpec((TOKENS, CUT), lambda t: (0, jnp.maximum(t - 1, 0)))
    return pl.pallas_call(
        kernel,
        grid=(cuts + 1,),
        in_specs=[ANY] * 3,
        out_specs=[block, block, block, pl.BlockSpec((D, TOKENS), lambda t: (0, 0))],
        out_shape=[shape(TOKENS, FF, dtype=F32), shape(TOKENS, FF, dtype=F32), shape(TOKENS, FF), shape(D, TOKENS)],
        scratch_shapes=[
            pltpu.VMEM((TOKENS, D), BF16), pltpu.VMEM((2, D, FF), BF16), dma, dma((2,)), dma((2,)), dma((2,)),
            dma((2, cuts)), dma((2, cuts)), dma((2, cuts)), dma((2, cuts)),
        ],
        name="fwd0_in",
        compiler_params=pltpu.CompilerParams(
            vmem_limit_bytes=VMEM, dimension_semantics=("arbitrary",), collective_id=2, has_side_effects=True
        ),
        cost_estimate=pl.CostEstimate(flops=2 * MM, bytes_accessed=TOKENS * FF * 10, transcendentals=TOKENS * FF),
    )(x, w_gate, w_up)


def forward_out(x, act, w_down):
    def kernel(x_ref, act_ref, w_ref, h_ref, a_ref, at_ref):
        for i in range(0, T1, SUB1):
            part = slice(i, i + SUB1)
            y = dot(act_ref[part, :], w_ref[...]).astype(BF16)
            h = (x_ref[part, :].astype(F32) + y.astype(F32)).astype(BF16)
            h_ref[part, :] = h
            wide = h.astype(F32)
            a = (wide * scale_of(wide)).astype(BF16)
            a_ref[part, :] = a
            at_ref[:, part] = a.T

    return call(
        kernel, "fwd0_out", TOKENS // T1,
        [rows(T1, D), rows(T1, FF), picked(0, FF, D)],
        [rows(T1, D), rows(T1, D), columns(D, T1)],
        [shape(TOKENS, D), shape(TOKENS, D), shape(D, TOKENS)],
        (), MM, TOKENS * (FF + 4 * D) * 2,
    )(x, act, w_down)


T3 = 512
STEP3 = 256


def gated(g, u, d):
    sig = jax.nn.sigmoid(g)
    s = g * sig
    d_gate = d * u * (sig + s * (1 - sig))
    return d_gate.astype(BF16), (d * s).astype(BF16), s


def middle(a, dy, w_gate, w_up, w_down):
    def kernel(a_ref, dy_ref, wg_ref, wu_ref, wd_ref, act_ref, dg_ref, du_ref, dyt_ref):
        a, dy = a_ref[...], dy_ref[...]
        dyt_ref[...] = dy.T
        step = STEP3
        for j in range(0, FF, step):
            g = dot(a, wg_ref[:, j : j + step])
            u = dot(a, wu_ref[:, j : j + step])
            d = dot_t(dy, wd_ref[j : j + step, :]).astype(BF16).astype(F32)
            dg_ref[:, j : j + step], du_ref[:, j : j + step], s = gated(g, u, d)
            act_ref[:, j : j + step] = (s * u).astype(BF16)

    return call(
        kernel, "mid1", TOKENS // T3,
        [rows(T3, D), rows(T3, D), picked(0, D, FF), picked(1, D, FF), picked(1, FF, D)],
        [rows(T3, FF), rows(T3, FF), rows(T3, FF), columns(D, T3)],
        [shape(TOKENS, FF)] * 3 + [shape(D, TOKENS)],
        (), 3 * MM, TOKENS * (3 * FF + 3 * D) * 2, TOKENS * FF,
    )(a, dy, w_gate, w_up, w_down)


T7 = 256
SUB7 = 256


def backward_in(dgate, dup, h, dy, gate, up, w_gate, w_up, w_down):
    def kernel(dg_ref, du_ref, h_ref, dy_ref, gate_ref, up_ref, wg_ref, wu_ref, wd_ref, dht_ref, odg_ref, odu_ref):
        for i in range(0, T7, SUB7):
            part = slice(i, i + SUB7)
            da = (dot_t(dg_ref[part, :], wg_ref[...]) + dot_t(du_ref[part, :], wu_ref[...])).astype(BF16).astype(F32)
            wide = h_ref[part, :].astype(F32)
            scale = scale_of(wide)
            along = jnp.mean(da * wide, -1, keepdims=True)
            dn = (scale * da - wide * (scale * scale * scale * along)).astype(BF16)
            dh = (dy_ref[part, :].astype(F32) + dn.astype(F32)).astype(BF16)
            dht_ref[:, part] = dh.T
            step = 512
            for j in range(0, FF, step):
                cols = slice(j, j + step)
                d = dot_t(dh, wd_ref[cols, :]).astype(BF16).astype(F32)
                odg_ref[part, cols], odu_ref[part, cols], _ = gated(gate_ref[part, cols], up_ref[part, cols], d)

    return call(
        kernel, "bwd_in", TOKENS // T7,
        [rows(T7, FF), rows(T7, FF), rows(T7, D), rows(T7, D), rows(T7, FF), rows(T7, FF), picked(0, D, FF), picked(1, D, FF), picked(0, FF, D)],
        [columns(D, T7), rows(T7, FF), rows(T7, FF)],
        [shape(D, TOKENS), shape(TOKENS, FF), shape(TOKENS, FF)],
        (), 3 * MM, TOKENS * (4 * FF + 3 * D) * 2 + TOKENS * FF * 8, TOKENS * FF,
    )(dgate, dup, h, dy, gate, up, w_gate, w_up, w_down)


DELAY = 11
CHUNKS = 5
UNIT = (RD, 128)


def weight_grads(lefts, rights):
    total = 6 * CHUNKS

    def kernel(*refs):
        left_refs, right_refs = refs[0:6], refs[6:12]
        out_refs = refs[12:15]
        (left, right, keep, a_send, a_recv, own, b_send, b_recv, mine, c_send, c_recv, d_send, d_recv,
         l_sem, r_sem, as_sem, ar_sem, bs_sem, br_sem, cs_sem, cr_sem, ds_sem, dr_sem) = refs[15:]
        t = pl.program_id(0)
        rep, r, s = lax.axis_index("rep"), lax.axis_index("r"), lax.axis_index("s")
        s_of, r_of = others(s), others(r)
        to_s = lambda k: (rep, r, s_of[k])
        to_r = lambda k: (rep, r_of[k], s)

        def left_copies(m, slot):
            at = r_of if m % 3 == 0 else s_of
            return [
                pltpu.make_async_copy(
                    left_refs[m].at[pl.ds(pl.multiple_of(at[k] * RD, RD), RD), :], left.at[slot, pl.ds(k * RD, RD), :], l_sem.at[slot, k]
                )
                for k in range(4)
            ]

        def right_copies(m, j, slot):
            if m % 3 == 0:
                at = [s_of[k] * RF + j * 128 for k in range(4)]
            else:
                at = [j * 512 + r_of[k] * 128 for k in range(4)]
            return [
                pltpu.make_async_copy(
                    right_refs[m].at[:, pl.ds(pl.multiple_of(at[k], 128), 128)], right.at[slot, :, pl.ds(k * 128, 128)], r_sem.at[slot, k]
                )
                for k in range(4)
            ]

        @pl.when(t == 0)
        def _():
            for c in left_copies(0, 0) + right_copies(0, 0, 0):
                c.start()
            barrier = pltpu.get_barrier_semaphore()
            for to in (to_s(1), to_s(2), to_r(1), to_r(2), to_r(3)):
                pl.semaphore_signal(barrier, inc=1, device_id=to, device_id_type=pl.DeviceIdType.MESH)
            pl.semaphore_wait(barrier, 5)

        def a_copy(c):
            return remote(a_send.at[c % 2], a_recv.at[c % 4], as_sem.at[c % 2], ar_sem.at[c % 4], to_s(1))

        def b_copy(c):
            return remote(b_send.at[c % 4], b_recv.at[c % 6], bs_sem.at[c % 4], br_sem.at[c % 6], to_s(2))

        def c_copies(c):
            return [
                remote(c_send.at[c % 4, k], c_recv.at[c % 6, k], cs_sem.at[c % 4, k], cr_sem.at[c % 6, k], to_r(k + 1))
                for k in range(3)
            ]

        def d_copies(c):
            return [
                remote(d_send.at[c % 4], d_recv.at[c % 6, k + 1], ds_sem.at[c % 4, k], dr_sem.at[c % 6, k], to_r(k + 1))
                for k in range(3)
            ]

        def live(c):
            return jnp.logical_and(c >= 0, c < total)

        @pl.when(live(t - 9))
        def _():
            for c in d_copies(t - 9):
                c.start()

        @pl.when(live(t - 6))
        def _():
            for c in c_copies(t - 6):
                c.start()

        @pl.when(live(t - 3))
        def _():
            b_copy(t - 3).start()

        @pl.when(live(t - 1))
        def _():
            a_copy(t - 1).start()

        nxt = t + 1
        for m in range(6):
            @pl.when(jnp.logical_and(nxt >= m * CHUNKS, nxt < (m + 1) * CHUNKS))
            def _(m=m):
                for c in right_copies(m, nxt - m * CHUNKS, nxt % 2):
                    c.start()

            if m and left_refs_of[m] != left_refs_of[m - 1]:
                @pl.when(nxt == m * CHUNKS)
                def _(m=m):
                    for c in left_copies(m, left_slot[m]):
                        c.start()

        @pl.when(live(t - 11))
        def _():
            c = t - 11
            for copy in d_copies(c):
                copy.wait()
            slot = c % 6
            for which in range(3):
                @pl.when((c // CHUNKS) % 3 == which)
                def _(which=which):
                    for k in range(4):
                        if which == 0:
                            out_refs[2][0, :, k * RD : (k + 1) * RD] = d_recv[slot, r_of[k]].T
                        else:
                            out_refs[which - 1][0, :, k * 128 : (k + 1) * 128] = d_recv[slot, r_of[k]]

        @pl.when(live(t - 8))
        def _():
            for copy in c_copies(t - 8):
                copy.wait()

        @pl.when(live(t - 5))
        def _():
            b_copy(t - 5).wait()

        @pl.when(live(t - 2))
        def _():
            a_copy(t - 2).wait()

        def whole_units():
            at = jnp.where(t < 8, 6, (t + 4) % 6)
            total_of = mine[t % 4]
            for k in range(3):
                total_of = total_of + c_recv[at, k].astype(F32)
            total_of = total_of.astype(BF16)
            d_send[t % 4] = total_of
            d_recv[(t + 4) % 6, 0] = total_of

        def chips_units():
            at = jnp.where(t < 5, 6, (t + 1) % 6)
            mine[(t + 3) % 4] = own[(t + 3) % 4, 0] + b_recv[at, 0].astype(F32)
            for k in range(3):
                c_send[(t + 3) % 4, k] = (own[(t + 3) % 4, k + 1] + b_recv[at, k + 1].astype(F32)).astype(BF16)

        def cores_units():
            for k in range(4):
                own[(t + 2) % 4, k] = keep[t % 2, k] + a_recv[(t + 2) % 4, k].astype(F32)
                b_send[(t + 2) % 4, k] = (keep[t % 2, k + 4] + a_recv[(t + 2) % 4, k + 4].astype(F32)).astype(BF16)

        for m in range(6):
            if m == 0 or left_refs_of[m] != left_refs_of[m - 1]:
                @pl.when(t == m * CHUNKS)
                def _(m=m):
                    for c in left_copies(m, left_slot[m]):
                        c.wait()

        @pl.when(t < total)
        def _():
            for c in right_copies(0, 0, t % 2):
                c.wait()

        def chunk(m_down, left_at):
            whole_units()
            chips_units()
            cores_units()
            out = dot(left[left_at], right[t % 2])
            for i in range(4):
                for k in range(4):
                    of_s, of_r = (k, i) if m_down else (i, k)
                    unit = out[i * RD : (i + 1) * RD, k * 128 : (k + 1) * 128]
                    if of_s % 2 == 0:
                        keep[t % 2, (of_s // 2) * 4 + of_r] = unit
                    else:
                        a_send[t % 2, (of_s // 2) * 4 + of_r] = unit.astype(BF16)

        @pl.when(jnp.logical_and(t < total, (t // CHUNKS) % 3 == 0))
        def _():
            chunk(True, left_at(t))

        @pl.when(jnp.logical_and(t < total, (t // CHUNKS) % 3 != 0))
        def _():
            chunk(False, left_at(t))

        @pl.when(jnp.logical_and(t >= total, t - 8 < total))
        def _():
            whole_units()

        @pl.when(jnp.logical_and(t >= total, t - 5 < total))
        def _():
            chips_units()

        @pl.when(jnp.logical_and(t >= total, t - 2 < total))
        def _():
            cores_units()

    left_refs_of = [0, 1, 1, 2, 3, 3]
    left_slot = [0, 1, 1, 0, 1, 1]

    def left_at(t):
        return jnp.minimum((t // CHUNKS) % 3, 1)

    def out_index(which):
        first = which * CHUNKS

        def at(t):
            c = t - DELAY
            late = c >= 3 * CHUNKS + first
            j = jnp.clip(jnp.where(late, c - 3 * CHUNKS - first, c - first), 0, CHUNKS - 1)
            return jnp.where(late, 0, 1), j

        return at

    def gate_up(which):
        at = out_index(which)

        def index(t):
            layer, j = at(t)
            return layer, 0, j

        return pl.BlockSpec((1, RD, 512), index)

    def down_index(t):
        layer, j = out_index(0)(t)
        return layer, j, 0

    dma = pltpu.SemaphoreType.DMA
    unit = lambda *n, dtype=BF16: pltpu.VMEM(n + UNIT, dtype)
    return pl.pallas_call(
        kernel,
        grid=(total + DELAY,),
        in_specs=[ANY] * 12,
        out_specs=[gate_up(1), gate_up(2), pl.BlockSpec((1, 128, D), down_index)],
        out_shape=[shape(2, RD, FF), shape(2, RD, FF), shape(2, RF, D)],
        scratch_shapes=[
            pltpu.VMEM((2, D, TOKENS), BF16), pltpu.VMEM((2, TOKENS, 512), BF16),
            unit(2, 8, dtype=F32), unit(2, 8), unit(4, 8), unit(4, 4, dtype=F32), unit(4, 4), unit(7, 4),
            unit(4, dtype=F32), unit(4, 3), unit(7, 3), unit(4), unit(6, 4),
            dma((2, 4)), dma((2, 4)), dma((2,)), dma((4,)), dma((4,)), dma((6,)),
            dma((4, 3)), dma((6, 3)), dma((4, 3)), dma((6, 3)),
        ],
        name="wgrads",
        compiler_params=pltpu.CompilerParams(
            vmem_limit_bytes=VMEM, dimension_semantics=("arbitrary",), collective_id=1, has_side_effects=True
        ),
        cost_estimate=pl.CostEstimate(flops=6 * MM, bytes_accessed=6 * TOKENS * (FF + D) * 2, transcendentals=0),
    )(*lefts, *rights)


def gathered(ws):
    r = lax.axis_index("r")
    n = ws[0].shape[0] // 4
    part = jnp.stack([lax.dynamic_slice_in_dim(w, r * n, n, 0) for w in ws])
    return lax.all_gather(part, ("s", "r"), axis=1, tiled=True)


def adamw(w, m, v, g):
    m = 0.9 * m + 0.1 * g
    v = 0.95 * v + 0.05 * g * g
    step = m * lax.rsqrt(v + 1e-8) + 0.1 * w
    return (w - 0.02 * step).astype(BF16), m, v


def solution(mesh):
    def step(x, dy, *arrays):
        weights, m, v = (arrays[i : i + 3] for i in (0, 3, 6))
        x, dy = x[0], dy[0]
        wg, wu, wd = weights
        downs = gathered([wd[0], wd[1]])
        ins = gathered([wg[1], wu[1]])
        gate0, up0, act0, a0t = forward_in(x, wg, wu)
        h1, a1, a1t = forward_out(x, act0, downs)
        act1, dgate1, dup1, dyt = middle(a1, dy, ins, ins, downs)
        dht, dgate0, dup0 = backward_in(dgate1, dup1, h1, dy, gate0, up0, ins, ins, downs)
        gradients = [g.astype(F32) for g in weight_grads([dyt, a1t, a1t, dht, a0t, a0t], [act1, dgate1, dup1, act0, dgate0, dup0])]
        new = [adamw(w.astype(F32), m, v, g) for w, m, v, g in zip(weights, m, v, gradients, strict=True)]
        return tuple(one[which] for which in range(3) for one in new)

    states, cut = P(("rep", "r", "s"), None, None), P(None, "s", None)
    return jax.shard_map(
        step,
        mesh=mesh,
        in_specs=(states, states) + (cut,) * 9,
        out_specs=(P("rep", "s", None),) * 9,
        check_vma=False,
    )
```
